512 devices in a mesh: layer: 8 (over z), row: 16 (over y, x_hi), col: 4 (over x_lo, core).
Axes of the slice: x: 4 (x_hi: 2, x_lo: 2; x = x_hi * 2 + x_lo), y: 8, z: 8, core: 2. Of those that a mesh axis runs over, the one named last changes fastest.
Arguments:
- left_matrix: bfloat16 [8192, 16384], P('row', ('layer', 'col')), may hold values from -6 to 6
- right_matrix: bfloat16 [16384, 8192], P(('layer', 'row'), 'col'), may hold values from -0.046875 to 0.046875
Outputs:
- product: bfloat16 [8192, 8192], P(('row', 'layer'), 'col')
The draws below stay inside these ranges and needn't reach their ends.
All inputs are finite; a program needn't handle non-finite values.
Results may differ from the reference program's by a relative error of at most 0.001.
Values may be sent and summed in bfloat16 or wider, within the bound.
No kernel may reach another device: no remote copies, remote signals or barrier semaphores. Data moves between devices by JAX's collectives and lax.ppermute only.
A program may use at most 64 MiB of HBM per device.

```python
import jax
import jax.numpy as jnp

K = 16384
N = 8192
M = 8192


def block_levels(stream_key, dims, split, smallest, top_value):
    level = 1.0
    for position, blocks in split:
        heights = jax.random.uniform(jax.random.fold_in(jax.random.fold_in(stream_key, 6), position), (blocks,), jnp.float32, smallest / len(split), top_value / len(split))
        level = level * jnp.repeat(jnp.exp(heights), dims[position] // blocks).reshape((-1,) + (1,) * (len(dims) - 1 - position))
    return level


def scatter_about(rng, dims, width, bound, pieces=(), kind=jnp.bfloat16):
    array = width * jax.random.normal(rng, dims, jnp.float32)
    if pieces:
        array = array * block_levels(rng, dims, pieces, -0.22, 0.18)
    return jnp.clip(array, -bound, bound).astype(kind)


def setup_inputs(seed: int = 0) -> dict:
    keys = jax.random.split(jax.random.key(seed), 3)
    left_matrix = scatter_about(keys[0], (M, K), 1.0, 6.0, ((0, 16), (1, 32)))
    right_matrix = scatter_about(keys[1], (K, N), K ** -0.5, 0.046875, ((0, 128), (1, 4)))
    return dict(left_matrix=left_matrix, right_matrix=right_matrix)


def reference(left_matrix, right_matrix):
    exact_sum = jnp.dot(left_matrix, right_matrix, preferred_element_type=jnp.float32)
    return exact_sum.astype(jnp.bfloat16)
```

```python
import jax
import jax.numpy as jnp
from jax import lax
from jax.sharding import Mesh
from jax.sharding import PartitionSpec as P


ROW = ("row_0", "row_1")
LAYER_ROW = ("layer", "row_0", "row_1")
ROW_LAYER = ("row_0", "row_1", "layer")
COL = ("col_0", "col_1")
CHUNKS = 4


def shifted(value, axes, by):
    size = 1
    for axis in axes:
        size *= lax.axis_size(axis)
    pairs = [(i, (i + by) % size) for i in range(size)]
    return lax.ppermute(value, axes, pairs)


def placed(whole, block, row, column):
    return lax.dynamic_update_slice(whole, block, (row, column))


def gathered_left(left):
    xs = ("row_1", "col_0")
    rows, cols = left.shape
    below = shifted(left, xs, 1)
    above = shifted(left, xs, -1)
    half = rows // 2
    far_top = shifted(below[:half], xs, 1)
    far_low = shifted(above[half:], xs, -1)
    far = jnp.concatenate([far_top, far_low], axis=0)
    x = lax.axis_index(xs)
    core = lax.axis_index("col_1")
    whole = jnp.zeros((2 * rows, 4 * cols), left.dtype)
    for block, at in ((left, x), (below, (x + 3) % 4), (above, (x + 1) % 4), (far, (x + 2) % 4)):
        other = shifted(block, ("col_1",), 1)
        whole = placed(whole, block, (at // 2) * rows, ((at % 2) * 2 + core) * cols)
        whole = placed(whole, other, (at // 2) * rows, ((at % 2) * 2 + 1 - core) * cols)
    return whole


def ring_gather(block, axis, more_up):
    size = lax.axis_size(axis)
    ups = size // 2 if more_up else size // 2 - 1
    downs = size - 1 - ups
    got = {0: block}
    up = down = block
    for step in range(1, max(ups, downs) + 1):
        if step <= ups:
            up = shifted(up, (axis,), 1)
            got[size - step] = up
        if step <= downs:
            down = shifted(down, (axis,), -1)
            got[step] = down
    return jnp.concatenate([got[i] for i in range(size)], axis=0)


def ring_scatter(parts, axis, more_up):
    size = lax.axis_size(axis)
    me = lax.axis_index(axis)

    def part(of):
        return lax.dynamic_index_in_dim(parts, (me + of) % size, axis=1, keepdims=False)

    ups = size // 2 if more_up else size // 2 - 1
    downs = size - 1 - ups
    up = down = None
    for step in range(max(ups, downs)):
        left = ups - step
        if left > 0:
            mine = part(left)
            up = shifted(mine if up is None else up + mine, (axis,), 1)
        left = downs - step
        if left > 0:
            mine = part(-left)
            down = shifted(mine if down is None else down + mine, (axis,), -1)
    return (part(0) + up) + down


def local(left_matrix, right_matrix):
    hi = lax.axis_index("row_1")
    y = lax.axis_index("row_0")
    depth, width = right_matrix.shape
    half = width // 2
    mine = lax.dynamic_slice(right_matrix, (0, hi * half), (depth, half))
    theirs = lax.dynamic_slice(right_matrix, (0, (1 - hi) * half), (depth, half))
    came = shifted(theirs, ("row_1",), 1)
    first = jnp.where(hi == 0, mine, came)
    second = jnp.where(hi == 0, came, mine)
    right = jnp.concatenate([first, second], axis=0)
    left = gathered_left(left_matrix)
    rows, inner = left.shape
    left = lax.dynamic_slice(jnp.concatenate([left, left], axis=1), (0, y * 2 * depth), (rows, inner))
    size = half // CHUNKS
    kept = []
    sent = []
    for chunk in range(CHUNKS):
        columns = ring_gather(right[:, chunk * size:(chunk + 1) * size], "row_0", chunk % 2 == 0)
        partial_value = jnp.dot(left, columns, preferred_element_type=jnp.float32)
        parts = partial_value.reshape(2, 8, rows // 16, size)
        summed = ring_scatter(parts, "layer", chunk % 2 == 0).astype(jnp.bfloat16)
        kept.append(lax.dynamic_index_in_dim(summed, hi, axis=0, keepdims=False))
        sent.append(shifted(lax.dynamic_index_in_dim(summed, 1 - hi, axis=0, keepdims=False), ("row_1",), 1))
    kept = jnp.concatenate(kept, axis=1)
    sent = jnp.concatenate(sent, axis=1)
    return jnp.concatenate([jnp.where(hi == 0, kept, sent), jnp.where(hi == 0, sent, kept)], axis=1)


def solution(mesh):
    split = Mesh(
        mesh.devices.reshape(mesh.shape["layer"], 8, 2, 2, 2),
        ("layer", "row_0", "row_1", "col_0", "col_1"),
    )
    in_specs = (P(ROW, ("layer", *COL)), P(LAYER_ROW, COL))
    out_specs = P(ROW_LAYER, COL)
    return jax.shard_map(local, mesh=split, in_specs=in_specs, out_specs=out_specs, check_vma=False)
```

```python
import jax
import jax.numpy as jnp
from jax import lax
from jax.experimental import pallas as pl
from jax.experimental.pallas import tpu as pltpu
from jax.sharding import Mesh
from jax.sharding import PartitionSpec as P


ROW = ("row_0", "row_1")
LAYER_ROW = ("layer", "row_0", "row_1")
ROW_LAYER = ("row_0", "row_1", "layer")
COL = ("col_0", "col_1")
CORE = "col_1"
X = ("row_1", "col_0")
Y = ("row_0",)
Z = ("layer",)
CHUNKS = (1024,)


def ring_size(axes):
    size = 1
    for axis in axes:
        size *= lax.axis_size(axis)
    return size


def turn(place):
    return 1 - 2 * (place % 2)


def exchange(value, axes, onward):
    size = ring_size(axes)
    pairs = []
    for at in range(size):
        for core in range(2):
            place = (at - core) % size
            to = place + turn(place) if onward else place - turn(place)
            pairs.append((at * 2 + core, (to + core) % size * 2 + core))
    return lax.ppermute(value, (*axes, CORE), pairs)


def swap_cores(value):
    return lax.ppermute(value, (CORE,), [(0, 1), (1, 0)])


def place_of(axes, core):
    size = ring_size(axes)
    place = lax.rem(lax.axis_index(axes) - core + size, size)
    return place, 1 - 2 * lax.rem(place, 2)


def product_kernel(a_own, a_far, a_own_2, a_far_2, b_0, b_1, b_2, b_3, *rest):
    outs, (a_all, b_all, a_sem, b_sem) = rest[:4], rest[4:]
    core = lax.axis_index(CORE)
    high = lax.axis_index("row_1")
    place, s = place_of(Z, core)
    slots = [4 + s, 4, 2 * s, 3 * s, -s, -2 * s, 0, s]
    layers = [lax.rem(place + core + slot + 16, 8) for slot in slots]
    edge = a_own.shape[1]
    piece = edge // 8
    for own, far, of in ((a_own, a_far, core), (a_own_2, a_far_2, 1 - core)):
        there, t = place_of(X, of)
        for number, by in enumerate((0, t, -t, -2 * t)):
            x = lax.rem(there + of + by + 8, 4)
            column = (lax.rem(x, 2) * 2 + of) * edge
            other = lax.rem(x // 2 + high, 2)
            source = own if number < 2 else far
            for slot in range(8):
                pltpu.make_async_copy(
                    source.at[pl.ds(pl.multiple_of((number % 2) * edge + layers[slot] * piece, piece), piece), :],
                    a_all.at[pl.ds(pl.multiple_of((slot * 2 + other) * piece, piece), piece), pl.ds(pl.multiple_of(column, edge), edge)],
                    a_sem,
                ).start()
    at, u = place_of(Y, core)
    block = b_0.shape[0] // 4
    for number, by in enumerate((0, u, -u, -2 * u, 2 * u, 3 * u, -3 * u, -4 * u)):
        y = lax.rem(at + core + by + 16, 8)
        source = (b_0, b_1, b_2, b_3)[number // 2]
        for other in range(2):
            row = (y * 2 + lax.rem(high + other, 2)) * block
            pltpu.make_async_copy(
                source.at[pl.ds((number % 2 * 2 + other) * block, block), :],
                b_all.at[pl.ds(pl.multiple_of(row, block), block), :],
                b_sem,
            ).start()
    pltpu.make_async_copy(a_all, a_all, a_sem).wait()
    pltpu.make_async_copy(b_all, b_all, b_sem).wait()
    rows = outs[0].shape[0]
    for part in range(4):
        outs[part][...] = jnp.dot(a_all[part * rows:(part + 1) * rows, :], b_all[...], preferred_element_type=jnp.float32)


def product(lefts, rights):
    depth = 4 * rights[0].shape[0]
    width = rights[0].shape[1]
    rows = lefts[0].shape[0]
    return pl.pallas_call(
        product_kernel,
        out_shape=[jax.ShapeDtypeStruct((rows // 4, width), jnp.float32)] * 4,
        in_specs=[pl.BlockSpec(memory_space=pltpu.HBM)] * 8,
        out_specs=[pl.BlockSpec(memory_space=pltpu.VMEM)] * 4,
        scratch_shapes=[
            pltpu.VMEM((rows, depth), jnp.bfloat16),
            pltpu.VMEM((depth, width), jnp.bfloat16),
            pltpu.SemaphoreType.DMA,
            pltpu.SemaphoreType.DMA,
        ],
        cost_estimate=pl.CostEstimate(flops=2 * rows * depth * width, transcendentals=0, bytes_accessed=2 * depth * (rows + width) + 4 * rows * width),
        name="product",
    )(*lefts, *rights)


def gathered_left(left):
    near = exchange(left, X, True)
    own = jnp.concatenate([left, near], axis=0)
    far = exchange(own, X, False)
    return own, far, swap_cores(own), swap_cores(far)


def gathered_right(right):
    near = exchange(right, Y, True)
    own = jnp.concatenate([right, near], axis=0)
    second = exchange(own, Y, False)
    third = exchange(second, Y, True)
    fourth = exchange(third, Y, False)
    return own, second, third, fourth


def scattered(parts):
    away, far, near, own = parts
    far = far + exchange(away, Z, False)
    near = near + exchange(far, Z, True)
    own = own + exchange(near, Z, False)
    half = own.shape[0] // 2
    return own[:half] + exchange(own[half:], Z, True)


def local(left_matrix, right_matrix):
    high = lax.axis_index("row_1")
    depth, width = right_matrix.shape
    half = width // 2
    lefts = None
    kept = []
    came = []
    start = 0
    for size in CHUNKS:
        mine = lax.dynamic_slice(right_matrix, (0, high * half + start), (depth, size))
        theirs = lax.dynamic_slice(right_matrix, (0, (1 - high) * half + start), (depth, size))
        theirs = lax.ppermute(theirs, ("row_1",), [(0, 1), (1, 0)])
        rights = gathered_right(jnp.concatenate([mine, theirs], axis=0))
        if lefts is None:
            lefts = gathered_left(left_matrix)
        summed = scattered(product(lefts, rights)).astype(jnp.bfloat16)
        rows = summed.shape[0] // 2
        kept.append(summed[:rows])
        came.append(lax.ppermute(summed[rows:], ("row_1",), [(0, 1), (1, 0)]))
        start += size
    kept = jnp.concatenate(kept, axis=1)
    came = jnp.concatenate(came, axis=1)
    return jnp.where(high == 0, jnp.concatenate([kept, came], axis=1), jnp.concatenate([came, kept], axis=1))


def solution(mesh):
    split = Mesh(
        mesh.devices.reshape(mesh.shape["layer"], 8, 2, 2, 2),
        ("layer", "row_0", "row_1", "col_0", "col_1"),
    )
    in_specs = (P(ROW, ("layer", *COL)), P(LAYER_ROW, COL))
    out_specs = P(ROW_LAYER, COL)
    return jax.shard_map(local, mesh=split, in_specs=in_specs, out_specs=out_specs, check_vma=False)
```

```python
import jax
import jax.numpy as jnp
from jax import lax
from jax.experimental import pallas as pl
from jax.experimental.pallas import tpu as pltpu
from jax.sharding import Mesh
from jax.sharding import PartitionSpec as P


ROW = ("row_0", "row_1")
LAYER_ROW = ("layer", "row_0", "row_1")
ROW_LAYER = ("row_0", "row_1", "layer")
COL = ("col_0", "col_1")
CORE = "col_1"
X = ("row_1", "col_0")
Y = ("row_0",)
Z = ("layer",)
PLACES_X = (0, 1, 3, 2)
PLACES_Y = (0, 1, 4, 5, 7, 6, 3, 2)


def ring_size(axes):
    size = 1
    for axis in axes:
        size *= lax.axis_size(axis)
    return size


def turn(place):
    return 1 - 2 * (place % 2)


def exchange(value, axes, onward):
    size = ring_size(axes)
    pairs = []
    for at in range(size):
        for core in range(2):
            place = (at - core) % size
            to = place + turn(place) if onward else place - turn(place)
            pairs.append((at * 2 + core, (to + core) % size * 2 + core))
    return lax.ppermute(value, (*axes, CORE), pairs)


def swap_cores(value):
    return lax.ppermute(value, (CORE,), [(0, 1), (1, 0)])


def place_of(axes, core):
    size = ring_size(axes)
    place = lax.rem(lax.axis_index(axes) - core + size, size)
    return place, 1 - 2 * lax.rem(place, 2)


def swap_high(value):
    return lax.ppermute(value, ("row_1",), [(0, 1), (1, 0)])


def entry(table, at):
    value = table[0]
    for index in range(1, len(table)):
        value = jnp.where(at == index, table[index], value)
    return value


def order_kernel(mine, theirs, out, sem):
    core = lax.axis_index(CORE)
    high = lax.axis_index("row_1")
    layer, s = place_of(Z, core)
    slots = (4 + s, 4, 2 * s, 3 * s, -s, -2 * s, 0, s)
    layers = [lax.rem(layer + core + slot + 16, 8) for slot in slots]
    at, u = place_of(Y, core)
    edge = mine.shape[1]
    piece = edge // 8
    for source, of in ((mine, core), (theirs, 1 - core)):
        there, t = place_of(X, of)
        for number, by in enumerate((0, t, -t, -2 * t)):
            x = lax.rem(there + of + by + 8, 4)
            other = lax.rem(x // 2 + high, 2)
            for side in range(2):
                y = (lax.rem(x, 2) * 2 + of) * 2 + side
                column = entry(PLACES_Y, lax.rem((y - core - at) * u + 16, 8)) * (edge // 2)
                for slot in range(8):
                    pltpu.make_async_copy(
                        source.at[pl.ds(pl.multiple_of(number * edge + layers[slot] * piece, piece), piece), pl.ds(side * (edge // 2), edge // 2)],
                        out.at[pl.ds(pl.multiple_of((slot * 2 + other) * piece, piece), piece), pl.ds(pl.multiple_of(column, edge // 2), edge // 2)],
                        sem,
                    ).start()
    pltpu.make_async_copy(out, out, sem).wait()


def ordered(mine, theirs):
    return pl.pallas_call(
        order_kernel,
        out_shape=jax.ShapeDtypeStruct((mine.shape[0] // 2, mine.shape[1] * 4), mine.dtype),
        in_specs=[pl.BlockSpec(memory_space=pltpu.HBM)] * 2,
        out_specs=pl.BlockSpec(memory_space=pltpu.VMEM),
        scratch_shapes=[pltpu.SemaphoreType.DMA],
        cost_estimate=pl.CostEstimate(flops=1 << 30, transcendentals=0, bytes_accessed=4 * mine.size * 2),
        name="order_left",
    )(mine, theirs)


def most_kernel(left, first, second, third, out):
    depth = first.shape[0]
    total = None
    for number, right in enumerate((first, second, third)):
        term = jnp.dot(left[:, number * depth:(number + 1) * depth], right[...], preferred_element_type=jnp.float32)
        total = term if total is None else total + term
    out[...] = total


def most(left, rights):
    rows, inner = left.shape
    depth, width = rights[0].shape
    return pl.pallas_call(
        most_kernel,
        grid=(4,),
        out_shape=jax.ShapeDtypeStruct((rows, width), jnp.float32),
        in_specs=[pl.BlockSpec((rows // 4, inner), lambda i: (i, 0))] + [pl.BlockSpec((depth, width), lambda i: (0, 0))] * 3,
        out_specs=pl.BlockSpec((rows // 4, width), lambda i: (i, 0)),
        cost_estimate=pl.CostEstimate(flops=6 * rows * depth * width, transcendentals=0, bytes_accessed=4 * rows * width),
        name="most",
    )(left, *rights)


def last_kernel(total, left, right, out):
    out[...] = (total[...] + jnp.dot(left[...], right[...], preferred_element_type=jnp.float32)).astype(out.dtype)


def last(total, left, right, first, count, dtype):
    rows, width = total.shape
    depth = right.shape[0]
    rows //= 4
    return pl.pallas_call(
        last_kernel,
        grid=(count,),
        out_shape=jax.ShapeDtypeStruct((rows * count, width), dtype),
        in_specs=[
            pl.BlockSpec((rows, width), lambda i: (i + first, 0)),
            pl.BlockSpec((rows, depth), lambda i: (i + first, 3)),
            pl.BlockSpec((depth, width), lambda i: (0, 0)),
        ],
        out_specs=pl.BlockSpec((rows, width), lambda i: (i, 0)),
        cost_estimate=pl.CostEstimate(flops=2 * count * rows * depth * width, transcendentals=0, bytes_accessed=8 * count * rows * width),
        name="last",
    )(total, left, right)


def local(left_matrix, right_matrix):
    high = lax.axis_index("row_1")
    depth, width = right_matrix.shape
    half = width // 2

    def by_high(mine, theirs):
        return [jnp.where(high == 0, mine, theirs), jnp.where(high == 0, theirs, mine)]

    mine = lax.dynamic_slice(right_matrix, (0, high * half), (depth, half))
    theirs = lax.dynamic_slice(right_matrix, (0, (1 - high) * half), (depth, half))
    came = swap_high(theirs)
    near = exchange(mine, Y, True)
    left_matrix, came = lax.optimization_barrier((left_matrix, came))
    near_came = exchange(came, Y, True)
    left_near = exchange(left_matrix, X, True)
    first = jnp.concatenate(by_high(mine, came) + by_high(near, near_came), axis=0)
    second = exchange(first, Y, False)
    left_own = jnp.concatenate([left_matrix, left_near], axis=0)
    left_far = exchange(left_own, X, False)
    third = exchange(second, Y, True)
    left_mine = jnp.concatenate([left_own, left_far], axis=0)
    left_theirs = swap_cores(left_mine)
    fourth = exchange(third, Y, False)
    left = ordered(left_mine, left_theirs)
    total = most(left, (first, second, third))
    away = last(total, left, fourth, 0, 1, jnp.float32)
    rest = last(total, left, fourth, 1, 3, jnp.float32)
    rows = away.shape[0]
    far, close, own = rest[:rows], rest[rows:2 * rows], rest[2 * rows:]
    far = far + exchange(away, Z, False)
    close = close + exchange(far, Z, True)
    own = own + exchange(close, Z, False)
    part = rows // 4
    out_sent = (own[part:2 * part] + exchange(own[3 * part:], Z, True)).astype(jnp.bfloat16)
    out_came = swap_high(out_sent)
    kept = (own[:part] + exchange(own[2 * part:3 * part], Z, True)).astype(jnp.bfloat16)
    return jnp.concatenate(by_high(kept, out_came), axis=1)


def solution(mesh):
    split = Mesh(
        mesh.devices.reshape(mesh.shape["layer"], 8, 2, 2, 2),
        ("layer", "row_0", "row_1", "col_0", "col_1"),
    )
    in_specs = (P(ROW, ("layer", *COL)), P(LAYER_ROW, COL))
    out_specs = P(ROW_LAYER, COL)
    return jax.shard_map(local, mesh=split, in_specs=in_specs, out_specs=out_specs, check_vma=False)
```

```python
import functools

import jax
import jax.numpy as jnp
from jax import lax
from jax.experimental import pallas as pl
from jax.experimental.pallas import tpu as pltpu
from jax.sharding import Mesh
from jax.sharding import PartitionSpec as P


ROW = ("row_0", "row_1")
LAYER_ROW = ("layer", "row_0", "row_1")
ROW_LAYER = ("row_0", "row_1", "layer")
COL = ("col_0", "col_1")
CORE = "col_1"
X = ("row_1", "col_0")
Y = ("row_0",)
Z = ("layer",)
PLACES_Y = (0, 1, 4, 5, 7, 6, 3, 2)


def ring_size(axes):
    size = 1
    for axis in axes:
        size *= lax.axis_size(axis)
    return size


def turn(place):
    return 1 - 2 * (place % 2)


def exchange(value, axes, onward):
    size = ring_size(axes)
    pairs = []
    for at in range(size):
        for core in range(2):
            place = (at - core) % size
            to = place + turn(place) if onward else place - turn(place)
            pairs.append((at * 2 + core, (to + core) % size * 2 + core))
    return lax.ppermute(value, (*axes, CORE), pairs)


def swap_cores(value):
    return lax.ppermute(value, (CORE,), [(0, 1), (1, 0)])


def place_of(axes, core):
    size = ring_size(axes)
    place = lax.rem(lax.axis_index(axes) - core + size, size)
    return place, 1 - 2 * lax.rem(place, 2)


def swap_high(value):
    return lax.ppermute(value, ("row_1",), [(0, 1), (1, 0)])


def entry(table, at):
    value = table[0]
    for index in range(1, len(table)):
        value = jnp.where(at == index, table[index], value)
    return value


def order_kernel(mine, theirs, out, sem):
    core = lax.axis_index(CORE)
    high = lax.axis_index("row_1")
    layer, s = place_of(Z, core)
    slots = (4 + s, 4, 2 * s, 3 * s, -s, -2 * s, 0, s)
    layers = [lax.rem(layer + core + slot + 16, 8) for slot in slots]
    at, u = place_of(Y, core)
    edge = mine.shape[1]
    piece = edge // 8
    for source, of in ((mine, core), (theirs, 1 - core)):
        there, t = place_of(X, of)
        for number, by in enumerate((0, t, -t, -2 * t)):
            x = lax.rem(there + of + by + 8, 4)
            other = lax.rem(x // 2 + high, 2)
            for side in range(2):
                y = (lax.rem(x, 2) * 2 + of) * 2 + side
                column = entry(PLACES_Y, lax.rem((y - core - at) * u + 16, 8)) * (edge // 2)
                for slot in range(8):
                    pltpu.make_async_copy(
                        source.at[pl.ds(pl.multiple_of(number * edge + layers[slot] * piece, piece), piece), pl.ds(side * (edge // 2), edge // 2)],
                        out.at[pl.ds(pl.multiple_of((slot * 2 + other) * piece, piece), piece), pl.ds(pl.multiple_of(column, edge // 2), edge // 2)],
                        sem,
                    ).start()
    pltpu.make_async_copy(out, out, sem).wait()


def ordered(mine, theirs):
    return pl.pallas_call(
        order_kernel,
        out_shape=pltpu.VMEM((mine.shape[0] // 2, mine.shape[1] * 4), mine.dtype),
        in_specs=[pl.BlockSpec(memory_space=pltpu.HBM)] * 2,
        out_specs=pl.BlockSpec(memory_space=pltpu.VMEM),
        scratch_shapes=[pltpu.SemaphoreType.DMA],
        cost_estimate=pl.CostEstimate(flops=1 << 30, transcendentals=0, bytes_accessed=4 * mine.size * 2),
        compiler_params=pltpu.CompilerParams(vmem_limit_bytes=8 << 20),
        name="order_left",
    )(mine, theirs)


def resident(value):
    return pltpu.with_memory_space_constraint(value, pltpu.VMEM)


IN_VMEM = pl.BlockSpec(memory_space=pltpu.VMEM)


def most_kernel(left, first, first_2, second, second_2, third, out):
    high = lax.axis_index("row_1")
    depth = third.shape[0]
    rows = left.shape[0] // 4
    block = depth // 4
    for part in range(4):
        at = pl.ds(part * rows, rows)
        total = jnp.dot(left[at, 2 * depth:3 * depth], third[...], preferred_element_type=jnp.float32)
        for number, pair in enumerate(((first, first_2), (second, second_2))):
            for side in range(2):
                for of in range(2):
                    column = number * depth + side * 2 * block + lax.rem(high + of, 2) * block
                    total += jnp.dot(left[at, pl.ds(pl.multiple_of(column, block), block)], pair[of][side * block:(side + 1) * block, :], preferred_element_type=jnp.float32)
        out[at, :] = total


def most(left, rights):
    rows = left.shape[0]
    depth, width = rights[-1].shape
    return pl.pallas_call(
        most_kernel,
        out_shape=pltpu.VMEM((rows, width), jnp.float32),
        in_specs=[IN_VMEM] * 6,
        out_specs=IN_VMEM,
        cost_estimate=pl.CostEstimate(flops=6 * rows * depth * width, transcendentals=0, bytes_accessed=4 * rows * width),
        compiler_params=pltpu.CompilerParams(vmem_limit_bytes=16 << 20),
        name="most",
    )(resident(left), *[resident(right) for right in rights])


def last_kernel(first, count, total, left, right, out):
    rows = total.shape[0] // 4
    depth = right.shape[0]
    for part in range(count):
        at = pl.ds((first + part) * rows, rows)
        out[part * rows:(part + 1) * rows, :] = total[at, :] + jnp.dot(left[at, 3 * depth:], right[...], preferred_element_type=jnp.float32)


def last(total, left, right, first, count):
    rows, width = total.shape
    depth = right.shape[0]
    return pl.pallas_call(
        functools.partial(last_kernel, first, count),
        out_shape=pltpu.VMEM((rows // 4 * count, width), jnp.float32),
        in_specs=[IN_VMEM] * 3,
        out_specs=IN_VMEM,
        cost_estimate=pl.CostEstimate(flops=rows // 2 * count * depth * width, transcendentals=0, bytes_accessed=2 * count * rows * width),
        compiler_params=pltpu.CompilerParams(vmem_limit_bytes=16 << 20),
        name="last",
    )(resident(total), resident(left), resident(right))


def step(left_matrix, right_matrix):
    high = lax.axis_index("row_1")
    depth, width = right_matrix.shape
    half = width // 2
    mine = lax.dynamic_slice(right_matrix, (0, high * half), (depth, half))
    theirs = lax.dynamic_slice(right_matrix, (0, (1 - high) * half), (depth, half))
    came = swap_high(theirs)
    near = exchange(mine, Y, True)
    first = jnp.concatenate([mine, near], axis=0)
    second = exchange(first, Y, False)
    near_came = exchange(came, Y, True)
    left_matrix, came = lax.optimization_barrier((left_matrix, came))
    first_2 = jnp.concatenate([came, near_came], axis=0)
    second_2 = exchange(first_2, Y, False)
    left_near = exchange(left_matrix, X, True)
    left_own = jnp.concatenate([left_matrix, left_near], axis=0)
    left_far = exchange(left_own, X, False)
    block = depth
    lower = jnp.where(high == 0, second, second_2)
    upper = jnp.where(high == 0, second_2, second)
    third_sent = jnp.concatenate([lower[:block], upper[:block], lower[block:], upper[block:]], axis=0)
    third = exchange(third_sent, Y, True)
    left_mine = jnp.concatenate([left_own, left_far], axis=0)
    left_theirs = swap_cores(left_mine)
    fourth = exchange(third, Y, False)
    left = ordered(left_mine, left_theirs)
    total = most(left, (first, first_2, second, second_2, third))
    away = last(total, left, fourth, 0, 1)
    rest = last(total, left, fourth, 1, 3)
    rows = away.shape[0]
    far, close, own = rest[:rows], rest[rows:2 * rows], rest[2 * rows:]
    far = far + exchange(away, Z, False)
    close = close + exchange(far, Z, True)
    own = own + exchange(close, Z, False)
    part = rows // 4
    out_sent = (own[part:2 * part] + exchange(own[3 * part:], Z, True)).astype(jnp.bfloat16)
    out_came = swap_high(out_sent)
    kept = (own[:part] + exchange(own[2 * part:3 * part], Z, True)).astype(jnp.bfloat16)
    return jnp.concatenate([jnp.where(high == 0, kept, out_came), jnp.where(high == 0, out_came, kept)], axis=1)


def solution(mesh):
    split = Mesh(
        mesh.devices.reshape(mesh.shape["layer"], 8, 2, 2, 2),
        ("layer", "row_0", "row_1", "col_0", "col_1"),
    )
    in_specs = (P(ROW, ("layer", *COL)), P(LAYER_ROW, COL))
    out_specs = P(ROW_LAYER, COL)
    return jax.shard_map(step, mesh=split, in_specs=in_specs, out_specs=out_specs, check_vma=False)
```

```python
import functools

import jax
import jax.numpy as jnp
from jax import lax
from jax.experimental import pallas as pl
from jax.experimental.pallas import tpu as pltpu
from jax.sharding import Mesh
from jax.sharding import PartitionSpec as P


ROW = ("row_0", "row_1")
LAYER_ROW = ("layer", "row_0", "row_1")
ROW_LAYER = ("row_0", "row_1", "layer")
COL = ("col_0", "col_1")
CORE = "col_1"
X = ("row_1", "col_0")
Y = ("row_0",)
Z = ("layer",)
PLACES_Y = (0, 1, 4, 5, 7, 6, 3, 2)


def ring_size(axes):
    size = 1
    for axis in axes:
        size *= lax.axis_size(axis)
    return size


def turn(place):
    return 1 - 2 * (place % 2)


def exchange(value, axes, onward):
    size = ring_size(axes)
    pairs = []
    for at in range(size):
        for core in range(2):
            place = (at - core) % size
            to = place + turn(place) if onward else place - turn(place)
            pairs.append((at * 2 + core, (to + core) % size * 2 + core))
    return lax.ppermute(value, (*axes, CORE), pairs)


def swap_cores(value):
    return lax.ppermute(value, (CORE,), [(0, 1), (1, 0)])


def place_of(axes, core):
    size = ring_size(axes)
    place = lax.rem(lax.axis_index(axes) - core + size, size)
    return place, 1 - 2 * lax.rem(place, 2)


def swap_high(value):
    return lax.ppermute(value, ("row_1",), [(0, 1), (1, 0)])


def entry(table, at):
    value = table[0]
    for index in range(1, len(table)):
        value = jnp.where(at == index, table[index], value)
    return value


def order_kernel(own, far, own_2, far_2, out, sem):
    core = lax.axis_index(CORE)
    high = lax.axis_index("row_1")
    layer, s = place_of(Z, core)
    slots = (4 + s, 4, 2 * s, 3 * s, -s, -2 * s, 0, s)
    layers = [lax.rem(layer + core + slot + 16, 8) for slot in slots]
    at, u = place_of(Y, core)
    edge = own.shape[1]
    piece = edge // 8
    for sources, of in (((own, far), core), ((own_2, far_2), 1 - core)):
        there, t = place_of(X, of)
        for number, by in enumerate((0, t, -t, -2 * t)):
            x = lax.rem(there + of + by + 8, 4)
            other = lax.rem(x // 2 + high, 2)
            source = sources[number // 2]
            for quarter in range(4):
                y = (lax.rem(x, 2) * 2 + of) * 2 + quarter // 2
                place = entry(PLACES_Y, lax.rem((y - core - at) * u + 16, 8))
                column = place // 2 * edge + lax.rem(high + quarter, 2) * (edge // 2) + lax.rem(place, 2) * (edge // 4)
                for slot in range(8):
                    pltpu.make_async_copy(
                        source.at[pl.ds(pl.multiple_of(number % 2 * edge + layers[slot] * piece, piece), piece), pl.ds(quarter * (edge // 4), edge // 4)],
                        out.at[pl.ds(pl.multiple_of((slot * 2 + other) * piece, piece), piece), pl.ds(pl.multiple_of(column, edge // 4), edge // 4)],
                        sem,
                    ).start()
    pltpu.make_async_copy(out, out, sem).wait()


def ordered(*pieces):
    rows, edge = pieces[0].shape
    return pl.pallas_call(
        order_kernel,
        out_shape=pltpu.VMEM((rows, edge * 4), pieces[0].dtype),
        in_specs=[pl.BlockSpec(memory_space=pltpu.HBM)] * 4,
        out_specs=pl.BlockSpec(memory_space=pltpu.VMEM),
        scratch_shapes=[pltpu.SemaphoreType.DMA],
        cost_estimate=pl.CostEstimate(flops=1 << 30, transcendentals=0, bytes_accessed=16 * rows * edge),
        compiler_params=pltpu.CompilerParams(vmem_limit_bytes=8 << 20),
        name="order_left",
    )(*pieces)


def resident(value):
    return pltpu.with_memory_space_constraint(value, pltpu.VMEM)


IN_VMEM = pl.BlockSpec(memory_space=pltpu.VMEM)


def most_kernel(left, first, first_2, second, second_2, third, out):
    rows = left.shape[0] // 4
    for part in range(4):
        at = pl.ds(part * rows, rows)
        total = None
        column = 0
        for right in (first, first_2, second, second_2, third):
            depth = right.shape[0]
            term = jnp.dot(left[at, column:column + depth], right[...], preferred_element_type=jnp.float32)
            total = term if total is None else total + term
            column += depth
        out[at, :] = total


def most(left, rights):
    rows = left.shape[0]
    depth, width = rights[-1].shape
    return pl.pallas_call(
        most_kernel,
        out_shape=pltpu.VMEM((rows, width), jnp.float32),
        in_specs=[IN_VMEM] * 6,
        out_specs=IN_VMEM,
        cost_estimate=pl.CostEstimate(flops=6 * rows * depth * width, transcendentals=0, bytes_accessed=4 * rows * width),
        compiler_params=pltpu.CompilerParams(vmem_limit_bytes=16 << 20),
        name="most",
    )(resident(left), *[resident(right) for right in rights])


def last_kernel(first, count, side, total, left, right, out):
    rows = total.shape[0] // 4
    depth = right.shape[0]
    for part in range(count):
        at = pl.ds((first + part) * rows, rows)
        width = right.shape[1]
        out[part * rows:(part + 1) * rows, :] = total[at, side * width:(side + 1) * width] + jnp.dot(left[at, 3 * depth:], right[...], preferred_element_type=jnp.float32)


def last(total, left, right, first, count, side):
    rows = total.shape[0]
    depth, width = right.shape
    return pl.pallas_call(
        functools.partial(last_kernel, first, count, side),
        out_shape=pltpu.VMEM((rows // 4 * count, width), jnp.float32),
        in_specs=[IN_VMEM] * 3,
        out_specs=IN_VMEM,
        cost_estimate=pl.CostEstimate(flops=rows // 2 * count * depth * width, transcendentals=0, bytes_accessed=2 * count * rows * width),
        compiler_params=pltpu.CompilerParams(vmem_limit_bytes=16 << 20),
        name="last",
    )(resident(total), resident(left), resident(right))


def step(left_matrix, right_matrix):
    high = lax.axis_index("row_1")
    depth, width = right_matrix.shape
    half = width // 2
    mine = lax.dynamic_slice(right_matrix, (0, high * half), (depth, half))
    theirs = lax.dynamic_slice(right_matrix, (0, (1 - high) * half), (depth, half))
    came = swap_high(theirs)
    near = exchange(mine, Y, True)
    first = jnp.concatenate([mine, near], axis=0)
    second = exchange(first, Y, False)
    near_came = exchange(came, Y, True)
    left_matrix, came = lax.optimization_barrier((left_matrix, came))
    first_2 = jnp.concatenate([came, near_came], axis=0)
    second_2 = exchange(first_2, Y, False)
    left_near = exchange(left_matrix, X, True)
    left_own = jnp.concatenate([left_matrix, left_near], axis=0)
    left_far = exchange(left_own, X, False)
    third_sent = jnp.concatenate([second, second_2], axis=0)
    third = exchange(third_sent, Y, True)
    own_theirs = swap_cores(left_own)
    far_theirs = swap_cores(left_far)
    middle = third.shape[1] // 2
    fourth = exchange(third[:, :middle], Y, False)
    fourth_right = exchange(third[:, middle:], Y, False)
    left = ordered(left_own, left_far, own_theirs, far_theirs)
    total = most(left, (first, first_2, second, second_2, third))
    kept = []
    out_came = []
    for side, columns in enumerate((fourth, fourth_right)):
        away = last(total, left, columns, 0, 1, side)
        rest = last(total, left, columns, 1, 3, side)
        rows = away.shape[0]
        far, close, own = rest[:rows], rest[rows:2 * rows], rest[2 * rows:]
        far = far + exchange(away, Z, False)
        close = close + exchange(far, Z, True)
        own = own + exchange(close, Z, False)
        own = (own[:rows // 2] + exchange(own[rows // 2:], Z, True)).astype(jnp.bfloat16)
        kept.append(own[:rows // 4])
        out_came.append(swap_high(own[rows // 4:]))
    kept = jnp.concatenate(kept, axis=1)
    out_came = jnp.concatenate(out_came, axis=1)
    return jnp.concatenate([jnp.where(high == 0, kept, out_came), jnp.where(high == 0, out_came, kept)], axis=1)


def solution(mesh):
    split = Mesh(
        mesh.devices.reshape(mesh.shape["layer"], 8, 2, 2, 2),
        ("layer", "row_0", "row_1", "col_0", "col_1"),
    )
    in_specs = (P(ROW, ("layer", *COL)), P(LAYER_ROW, COL))
    out_specs = P(ROW_LAYER, COL)
    return jax.shard_map(step, mesh=split, in_specs=in_specs, out_specs=out_specs, check_vma=False)
```

```python
import functools

import jax
import jax.numpy as jnp
from jax import lax
from jax.experimental import pallas as pl
from jax.experimental.pallas import tpu as pltpu
from jax.sharding import Mesh
from jax.sharding import PartitionSpec as P


ROW = ("row_0", "row_1")
LAYER_ROW = ("layer", "row_0", "row_1")
ROW_LAYER = ("row_0", "row_1", "layer")
COL = ("col_0", "col_1")
CORE = "col_1"
X = ("row_1", "col_0")
Y = ("row_0",)
Z = ("layer",)
EXTRA = 16
STRETCH = 2.3
PLACES_Y = (0, 1, 4, 5, 7, 6, 3, 2)


def ring_size(axes):
    size = 1
    for axis in axes:
        size *= lax.axis_size(axis)
    return size


def turn(place):
    return 1 - 2 * (place % 2)


def exchange(value, axes, onward):
    size = ring_size(axes)
    pairs = []
    for at in range(size):
        for core in range(2):
            place = (at - core) % size
            to = place + turn(place) if onward else place - turn(place)
            pairs.append((at * 2 + core, (to + core) % size * 2 + core))
    return lax.ppermute(value, (*axes, CORE), pairs)


def swap_cores(value):
    return lax.ppermute(value, (CORE,), [(0, 1), (1, 0)])


def place_of(axes, core):
    size = ring_size(axes)
    place = lax.rem(lax.axis_index(axes) - core + size, size)
    return place, 1 - 2 * lax.rem(place, 2)


def swap_high(value):
    return lax.ppermute(value, ("row_1",), [(0, 1), (1, 0)])


def entry(table, at):
    value = table[0]
    for index in range(1, len(table)):
        value = jnp.where(at == index, table[index], value)
    return value


def order_kernel(own, far, own_2, far_2, out, sem):
    core = lax.axis_index(CORE)
    high = lax.axis_index("row_1")
    layer, s = place_of(Z, core)
    slots = (4 + s, 4, 2 * s, 3 * s, -s, -2 * s, 0, s)
    layers = [lax.rem(layer + core + slot + 16, 8) for slot in slots]
    at, u = place_of(Y, core)
    edge = own.shape[1]
    piece = edge // 8
    for sources, of in (((own, far), core), ((own_2, far_2), 1 - core)):
        there, t = place_of(X, of)
        for number, by in enumerate((0, t, -t, -2 * t)):
            x = lax.rem(there + of + by + 8, 4)
            other = lax.rem(x // 2 + high, 2)
            source = sources[number // 2]
            for quarter in range(4):
                y = (lax.rem(x, 2) * 2 + of) * 2 + quarter // 2
                place = entry(PLACES_Y, lax.rem((y - core - at) * u + 16, 8))
                column = place // 2 * edge + lax.rem(high + quarter, 2) * (edge // 2) + lax.rem(place, 2) * (edge // 4)
                for slot in range(8):
                    pltpu.make_async_copy(
                        source.at[pl.ds(pl.multiple_of(number % 2 * edge + layers[slot] * piece, piece), piece), pl.ds(quarter * (edge // 4), edge // 4)],
                        out.at[pl.ds(pl.multiple_of((slot * 2 + other) * piece, piece), piece), pl.ds(pl.multiple_of(column, edge // 4), edge // 4)],
                        sem,
                    ).start()
    pltpu.make_async_copy(out, out, sem).wait()


def ordered(*pieces):
    rows, edge = pieces[0].shape
    return pl.pallas_call(
        order_kernel,
        out_shape=pltpu.VMEM((rows, edge * 4), pieces[0].dtype),
        in_specs=[pl.BlockSpec(memory_space=pltpu.HBM)] * 4,
        out_specs=pl.BlockSpec(memory_space=pltpu.VMEM),
        scratch_shapes=[pltpu.SemaphoreType.DMA],
        cost_estimate=pl.CostEstimate(flops=1 << 30, transcendentals=0, bytes_accessed=16 * rows * edge),
        compiler_params=pltpu.CompilerParams(vmem_limit_bytes=8 << 20),
        name="order_left",
    )(*pieces)


def resident(value):
    return pltpu.with_memory_space_constraint(value, pltpu.VMEM)


IN_VMEM = pl.BlockSpec(memory_space=pltpu.VMEM)


def most_kernel(left, first, first_2, second, second_2, third, out):
    rows = left.shape[0] // 4
    for part in range(4):
        at = pl.ds(part * rows, rows)
        total = None
        column = 0
        for right in (first, first_2, second, second_2, third):
            depth = right.shape[0]
            term = jnp.dot(left[at, column:column + depth], right[...], preferred_element_type=jnp.float32)
            total = term if total is None else total + term
            column += depth
        out[at, :] = total


def most(left, rights):
    rows = left.shape[0]
    depth, width = rights[-1].shape
    return pl.pallas_call(
        most_kernel,
        out_shape=pltpu.VMEM((rows, width), jnp.float32),
        in_specs=[IN_VMEM] * 6,
        out_specs=IN_VMEM,
        cost_estimate=pl.CostEstimate(flops=6 * rows * depth * width, transcendentals=0, bytes_accessed=4 * rows * width),
        compiler_params=pltpu.CompilerParams(vmem_limit_bytes=16 << 20),
        name="most",
    )(resident(left), *[resident(right) for right in rights])


def coded(value, out):
    rows = value.shape[0]
    square = jnp.sum(jnp.sum(value * value, axis=0, keepdims=True), axis=1, keepdims=True) / value.size
    power = jnp.clip(jnp.floor(0.5 * jnp.log2(jnp.maximum(square, 1e-37))) - 1.0, -100.0, 100.0)
    unit = jnp.abs(value) * jnp.exp2(-power)
    grown = jnp.exp2(STRETCH * jnp.log2(unit + jnp.sqrt(unit * unit + 1.0)) - 14.0)
    out[:rows, :] = jnp.where(value < 0.0, -grown, grown)
    out[rows:, :] = jnp.broadcast_to(power, (EXTRA, out.shape[1]))


def decoded(value):
    rows = value.shape[0] - EXTRA
    code = value[:rows, :]
    grown = jnp.exp2((jnp.log2(jnp.abs(code)) + 14.0) * (1.0 / STRETCH))
    unit = 0.5 * (grown - 1.0 / grown) * jnp.exp2(value[rows:rows + 1, :])
    return jnp.where(code < 0.0, -unit, unit)


def part_of(total, left, right, part, side):
    rows = total.shape[0] // 4
    depth, width = right.shape
    at = pl.ds(part * rows, rows)
    return total[at, side * width:(side + 1) * width] + jnp.dot(left[at, 3 * depth:], right[...], preferred_element_type=jnp.float32)


def away_kernel(side, total, left, right, out):
    coded(part_of(total, left, right, 0, side), out)


def rest_kernel(side, total, left, right, out):
    rows = total.shape[0] // 4
    for part in range(3):
        out[part * rows:(part + 1) * rows, :] = part_of(total, left, right, part + 1, side)


def last(kernel, rows, total, left, right, side):
    depth, width = right.shape
    flops = 2 * sum(rows) * depth * width
    return pl.pallas_call(
        functools.partial(kernel, side),
        out_shape=[pltpu.VMEM((count, width), jnp.float32) for count in rows],
        in_specs=[IN_VMEM] * 3,
        out_specs=[IN_VMEM] * len(rows),
        cost_estimate=pl.CostEstimate(flops=flops, transcendentals=0, bytes_accessed=8 * sum(rows) * width),
        compiler_params=pltpu.CompilerParams(vmem_limit_bytes=16 << 20),
    )(resident(total), resident(left), resident(right))


def more_kernel(first, base, value, out):
    rows = value.shape[0] - EXTRA
    total = base[first:first + rows, :] + decoded(value)
    if out.shape[0] > rows:
        coded(total, out)
    else:
        out[...] = total


def more(base, first, value, extra):
    rows, width = value.shape
    return pl.pallas_call(
        functools.partial(more_kernel, first),
        out_shape=pltpu.VMEM((rows - EXTRA + extra, width), jnp.float32),
        in_specs=[IN_VMEM] * 2,
        out_specs=IN_VMEM,
        cost_estimate=pl.CostEstimate(flops=20 * value.size, transcendentals=4 * value.size, bytes_accessed=12 * value.size),
        compiler_params=pltpu.CompilerParams(vmem_limit_bytes=8 << 20),
        name="more",
    )(resident(base), resident(value.astype(jnp.float32)))


def sent(value, onward):
    return exchange(value.astype(jnp.float16), Z, onward)


def step(left_matrix, right_matrix):
    high = lax.axis_index("row_1")
    depth, width = right_matrix.shape
    half = width // 2
    mine = lax.dynamic_slice(right_matrix, (0, high * half), (depth, half))
    theirs = lax.dynamic_slice(right_matrix, (0, (1 - high) * half), (depth, half))
    came = swap_high(theirs)
    near = exchange(mine, Y, True)
    first = jnp.concatenate([mine, near], axis=0)
    second = exchange(first, Y, False)
    near_came = exchange(came, Y, True)
    left_matrix, came = lax.optimization_barrier((left_matrix, came))
    first_2 = jnp.concatenate([came, near_came], axis=0)
    second_2 = exchange(first_2, Y, False)
    left_near = exchange(left_matrix, X, True)
    left_own = jnp.concatenate([left_matrix, left_near], axis=0)
    left_far = exchange(left_own, X, False)
    third_sent = jnp.concatenate([second, second_2], axis=0)
    third = exchange(third_sent, Y, True)
    own_theirs = swap_cores(left_own)
    far_theirs = swap_cores(left_far)
    middle = third.shape[1] // 2
    fourth = exchange(third[:, :middle], Y, False)
    fourth_right = exchange(third[:, middle:], Y, False)
    left = ordered(left_own, left_far, own_theirs, far_theirs)
    total = most(left, (first, first_2, second, second_2, third))
    kept = []
    for side, columns in enumerate((fourth, fourth_right)):
        rows = total.shape[0] // 4
        away, = last(away_kernel, (rows + EXTRA,), total, left, columns, side)
        rest, = last(rest_kernel, (3 * rows,), total, left, columns, side)
        far = more(rest, 0, sent(away, False), EXTRA)
        close = more(rest, rows, sent(far, True), EXTRA)
        own = more(rest, 2 * rows, sent(close, False), 0)
        own = (own[:rows // 2] + exchange(own[rows // 2:], Z, True)).astype(jnp.bfloat16)
        kept.append(own)
    whole = jnp.concatenate(kept, axis=1)
    out_came = swap_high(whole[rows // 4:])
    whole = whole[:rows // 4]
    return jnp.concatenate([jnp.where(high == 0, whole, out_came), jnp.where(high == 0, out_came, whole)], axis=1)


def solution(mesh):
    split = Mesh(
        mesh.devices.reshape(mesh.shape["layer"], 8, 2, 2, 2),
        ("layer", "row_0", "row_1", "col_0", "col_1"),
    )
    in_specs = (P(ROW, ("layer", *COL)), P(LAYER_ROW, COL))
    out_specs = P(ROW_LAYER, COL)
    return jax.shard_map(step, mesh=split, in_specs=in_specs, out_specs=out_specs, check_vma=False)
```

```python
import functools

import jax
import jax.numpy as jnp
from jax import lax
from jax.experimental import pallas as pl
from jax.experimental.pallas import tpu as pltpu
from jax.sharding import Mesh
from jax.sharding import PartitionSpec as P


ROW = ("row_0", "row_1")
LAYER_ROW = ("layer", "row_0", "row_1")
ROW_LAYER = ("row_0", "row_1", "layer")
COL = ("col_0", "col_1")
CORE = "col_1"
X = ("row_1", "col_0")
Y = ("row_0",)
Z = ("layer",)
EXTRA = 16
STRETCH = 2.3
PLACES_Y = (0, 1, 4, 5, 7, 6, 3, 2)


def ring_size(axes):
    size = 1
    for axis in axes:
        size *= lax.axis_size(axis)
    return size


def turn(place):
    return 1 - 2 * (place % 2)


def exchange(value, axes, onward):
    size = ring_size(axes)
    pairs = []
    for at in range(size):
        for core in range(2):
            place = (at - core) % size
            to = place + turn(place) if onward else place - turn(place)
            pairs.append((at * 2 + core, (to + core) % size * 2 + core))
    return lax.ppermute(value, (*axes, CORE), pairs)


def swap_cores(value):
    return lax.ppermute(value, (CORE,), [(0, 1), (1, 0)])


def place_of(axes, core):
    size = ring_size(axes)
    place = lax.rem(lax.axis_index(axes) - core + size, size)
    return place, 1 - 2 * lax.rem(place, 2)


def swap_high(value):
    return lax.ppermute(value, ("row_1",), [(0, 1), (1, 0)])


def entry(table, at):
    value = table[0]
    for index in range(1, len(table)):
        value = jnp.where(at == index, table[index], value)
    return value


def order_kernel(own, far, own_2, far_2, out, sem):
    core = lax.axis_index(CORE)
    high = lax.axis_index("row_1")
    layer, s = place_of(Z, core)
    slots = (4 + s, 4, 2 * s, 3 * s, -s, -2 * s, 0, s)
    layers = [lax.rem(layer + core + slot + 16, 8) for slot in slots]
    at, u = place_of(Y, core)
    edge = own.shape[1]
    piece = edge // 8
    for sources, of in (((own, far), core), ((own_2, far_2), 1 - core)):
        there, t = place_of(X, of)
        for number, by in enumerate((0, t, -t, -2 * t)):
            x = lax.rem(there + of + by + 8, 4)
            other = lax.rem(x // 2 + high, 2)
            source = sources[number // 2]
            for quarter in range(4):
                y = (lax.rem(x, 2) * 2 + of) * 2 + quarter // 2
                place = entry(PLACES_Y, lax.rem((y - core - at) * u + 16, 8))
                column = place // 2 * edge + lax.rem(high + quarter, 2) * (edge // 2) + lax.rem(place, 2) * (edge // 4)
                for slot in range(8):
                    pltpu.make_async_copy(
                        source.at[pl.ds(pl.multiple_of(number % 2 * edge + layers[slot] * piece, piece), piece), pl.ds(quarter * (edge // 4), edge // 4)],
                        out.at[pl.ds(pl.multiple_of((slot * 2 + other) * piece, piece), piece), pl.ds(pl.multiple_of(column, edge // 4), edge // 4)],
                        sem,
                    ).start()
    pltpu.make_async_copy(out, out, sem).wait()


def ordered(*pieces):
    rows, edge = pieces[0].shape
    return pl.pallas_call(
        order_kernel,
        out_shape=pltpu.VMEM((rows, edge * 4), pieces[0].dtype),
        in_specs=[pl.BlockSpec(memory_space=pltpu.HBM)] * 4,
        out_specs=pl.BlockSpec(memory_space=pltpu.VMEM),
        scratch_shapes=[pltpu.SemaphoreType.DMA],
        cost_estimate=pl.CostEstimate(flops=1 << 30, transcendentals=0, bytes_accessed=16 * rows * edge),
        compiler_params=pltpu.CompilerParams(vmem_limit_bytes=8 << 20),
        name="order_left",
    )(*pieces)


def resident(value):
    return pltpu.with_memory_space_constraint(value, pltpu.VMEM)


IN_VMEM = pl.BlockSpec(memory_space=pltpu.VMEM)


def most_kernel(left, first, first_2, second, second_2, third, out):
    rows = left.shape[0] // 4
    for part in range(4):
        at = pl.ds(part * rows, rows)
        total = None
        column = 0
        for right in (first, first_2, second, second_2, third):
            depth = right.shape[0]
            term = jnp.dot(left[at, column:column + depth], right[...], preferred_element_type=jnp.float32)
            total = term if total is None else total + term
            column += depth
        out[at, :] = total


def most(left, rights):
    rows = left.shape[0]
    depth, width = rights[-1].shape
    return pl.pallas_call(
        most_kernel,
        out_shape=pltpu.VMEM((rows, width), jnp.float32),
        in_specs=[IN_VMEM] * 6,
        out_specs=IN_VMEM,
        cost_estimate=pl.CostEstimate(flops=6 * rows * depth * width, transcendentals=0, bytes_accessed=4 * rows * width),
        compiler_params=pltpu.CompilerParams(vmem_limit_bytes=16 << 20),
        name="most",
    )(resident(left), *[resident(right) for right in rights])


SLAB = 32


def level(square, count):
    square = jnp.sum(square, axis=1, keepdims=True) / count
    return jnp.clip(jnp.floor(0.5 * jnp.log2(jnp.maximum(square, 1e-37))) - 1.0, -100.0, 100.0)


def code(out, rows, square):
    power = level(square, rows * out.shape[1])
    scale = jnp.exp2(-power)

    def slab(number, carry):
        at = pl.ds(pl.multiple_of(number * SLAB, SLAB), SLAB)
        value = out[at, :]
        unit = jnp.abs(value) * scale
        more = unit * unit + 1.0
        grown = jnp.exp2(STRETCH * jnp.log2(unit + more * lax.rsqrt(more)) - 14.0)
        out[at, :] = jnp.where(value < 0.0, -grown, grown)
        return carry

    lax.fori_loop(0, rows // SLAB, slab, 0)
    out[rows:, :] = jnp.broadcast_to(power, (EXTRA, out.shape[1]))


def decoded(value, scale):
    lift = (jnp.log2(jnp.abs(value)) + 14.0) * (1.0 / STRETCH)
    unit = (jnp.exp2(lift) - jnp.exp2(-lift)) * scale
    return jnp.where(value < 0.0, -unit, unit)


def part_of(total, left, right, part, start):
    rows = total.shape[0] // 4
    depth, width = right.shape
    at = pl.ds(part * rows, rows)
    return total[at, start:start + width] + jnp.dot(left[at, 3 * depth:], right[...], preferred_element_type=jnp.float32)


def away_kernel(start, total, left, right, out):
    value = part_of(total, left, right, 0, start)
    rows = value.shape[0]
    out[:rows, :] = value
    code(out, rows, jnp.sum(value * value, axis=0, keepdims=True))


def rest_kernel(start, total, left, right, out):
    rows = total.shape[0] // 4
    for part in range(3):
        out[part * rows:(part + 1) * rows, :] = part_of(total, left, right, part + 1, start)


def last(kernel, rows, total, left, right, start):
    depth, width = right.shape
    flops = 2 * sum(rows) * depth * width
    return pl.pallas_call(
        functools.partial(kernel, start),
        out_shape=[pltpu.VMEM((count, width), jnp.float32) for count in rows],
        in_specs=[IN_VMEM] * 3,
        out_specs=[IN_VMEM] * len(rows),
        cost_estimate=pl.CostEstimate(flops=flops, transcendentals=0, bytes_accessed=8 * sum(rows) * width),
        compiler_params=pltpu.CompilerParams(vmem_limit_bytes=16 << 20),
    )(resident(total), resident(left), resident(right))


def more_kernel(first, base, value, out):
    rows = value.shape[0] - EXTRA
    scale = 0.5 * jnp.exp2(value[rows:rows + 1, :])

    def slab(number, square):
        start = pl.multiple_of(number * SLAB, SLAB)
        total = base[pl.ds(first + start, SLAB), :] + decoded(value[pl.ds(start, SLAB), :], scale)
        out[pl.ds(start, SLAB), :] = total
        return square + jnp.sum(total * total, axis=0, keepdims=True)

    square = lax.fori_loop(0, rows // SLAB, slab, jnp.zeros((1, out.shape[1]), jnp.float32))
    if out.shape[0] > rows:
        code(out, rows, square)


def more(base, first, value, extra):
    rows, width = value.shape
    return pl.pallas_call(
        functools.partial(more_kernel, first),
        out_shape=pltpu.VMEM((rows - EXTRA + extra, width), jnp.float32),
        in_specs=[IN_VMEM] * 2,
        out_specs=IN_VMEM,
        cost_estimate=pl.CostEstimate(flops=20 * value.size, transcendentals=4 * value.size, bytes_accessed=12 * value.size),
        compiler_params=pltpu.CompilerParams(vmem_limit_bytes=8 << 20),
        name="more",
    )(resident(base), resident(value.astype(jnp.float32)))


def sent(value, onward):
    return exchange(value.astype(jnp.float16), Z, onward)


def step(left_matrix, right_matrix):
    high = lax.axis_index("row_1")
    depth, width = right_matrix.shape
    half = width // 2
    mine = lax.dynamic_slice(right_matrix, (0, high * half), (depth, half))
    theirs = lax.dynamic_slice(right_matrix, (0, (1 - high) * half), (depth, half))
    came = swap_high(theirs)
    near = exchange(mine, Y, True)
    first = jnp.concatenate([mine, near], axis=0)
    second = exchange(first, Y, False)
    near_came = exchange(came, Y, True)
    left_matrix, came = lax.optimization_barrier((left_matrix, came))
    first_2 = jnp.concatenate([came, near_came], axis=0)
    second_2 = exchange(first_2, Y, False)
    left_near = exchange(left_matrix, X, True)
    left_own = jnp.concatenate([left_matrix, left_near], axis=0)
    left_far = exchange(left_own, X, False)
    third_sent = jnp.concatenate([second, second_2], axis=0)
    third = exchange(third_sent, Y, True)
    own_theirs = swap_cores(left_own)
    far_theirs = swap_cores(left_far)
    middle = 640
    fourth = exchange(third[:, :middle], Y, False)
    fourth_right = exchange(third[:, middle:], Y, False)
    left = ordered(left_own, left_far, own_theirs, far_theirs)
    total = most(left, (first, first_2, second, second_2, third))
    kept = []
    for side, columns in enumerate((fourth, fourth_right)):
        rows = total.shape[0] // 4
        away, = last(away_kernel, (rows + EXTRA,), total, left, columns, side * middle)
        rest, = last(rest_kernel, (3 * rows,), total, left, columns, side * middle)
        far = more(rest, 0, sent(away, False), EXTRA)
        close = more(rest, rows, sent(far, True), EXTRA)
        own = more(rest, 2 * rows, sent(close, False), 0)
        own = (own[:rows // 2] + exchange(own[rows // 2:], Z, True)).astype(jnp.bfloat16)
        kept.append(own)
    whole = jnp.concatenate(kept, axis=1)
    out_came = swap_high(whole[rows // 4:])
    whole = whole[:rows // 4]
    return jnp.concatenate([jnp.where(high == 0, whole, out_came), jnp.where(high == 0, out_came, whole)], axis=1)


def solution(mesh):
    split = Mesh(
        mesh.devices.reshape(mesh.shape["layer"], 8, 2, 2, 2),
        ("layer", "row_0", "row_1", "col_0", "col_1"),
    )
    in_specs = (P(ROW, ("layer", *COL)), P(LAYER_ROW, COL))
    out_specs = P(ROW_LAYER, COL)
    return jax.shard_map(step, mesh=split, in_specs=in_specs, out_specs=out_specs, check_vma=False)
```
